32 devices in a mesh: rows: 8 (over z, x), bal: 4 (over y, core).
Axes of the slice: x: 2, y: 2, z: 4, core: 2. Of those that a mesh axis runs over, the one named last changes fastest.
Arguments:
- embeddings: bfloat16 [16384, 1024], P(('rows', 'bal')), may hold values from -60 to 60
- cluster_blocks: int32 [16], replicated, may hold values from 1 to 4, as said below
Outputs:
- row_max: float32 [16384], P(('rows', 'bal'))
The draws below stay inside these ranges and needn't reach their ends.
Inputs may be any that keep to these rules, and one draw needn't show every extreme that they name: `cluster_blocks`: the sizes sum to 32; at least one cluster has exactly 4 blocks.
All inputs are finite; a program needn't handle non-finite values.
Results may differ from the reference program's by a relative error of at most 0.00051.
Values may be sent and summed in bfloat16 or wider, within the bound.
A program may use at most 64 MiB of HBM per device.

```python
import jax
import jax.numpy as jnp
from jax import lax

D = 1024
BLOCK = 512
MAXB = 4
NBLK = 32
NCL = 16


def fill_segment(sizes, key, first, last, extra):
    slots = jnp.arange(NCL, dtype=jnp.int32)
    picks = jax.random.randint(jax.random.fold_in(key, 22), (extra,), 0, NCL)
    shuffled = jax.random.permutation(jax.random.fold_in(key, 23), NCL).astype(jnp.int32)
    outside = ((slots < first) | (slots >= last)).astype(jnp.int32)

    def place(counts, pick):
        biased = shuffled[pick * pick // NCL]
        distance = (slots - biased) % NCL
        blocked = jnp.maximum((counts >= MAXB).astype(jnp.int32), outside)
        target = jnp.argmin(distance + NCL * blocked)
        return (counts.at[target].add(1), 0)
    sizes, _ = lax.scan(place, sizes, picks)
    return sizes


def cluster_sizes(key):
    special = NCL // 2
    sizes = jnp.ones((NCL,), jnp.int32).at[special].set(MAXB)
    front_extra = NBLK // 2 - 2 - special
    back_extra = NBLK - NBLK // 2 - 2 - (NCL - special - 1)
    sizes = fill_segment(sizes, jax.random.fold_in(key, 41), 0, special, front_extra)
    sizes = fill_segment(sizes, jax.random.fold_in(key, 42), special + 1, NCL, back_extra)
    return sizes


def draw_cluster_blocks(key, part):
    return cluster_sizes(jax.random.fold_in(key, 7))


def draw_embeddings(key, part):
    sizes = cluster_sizes(jax.random.fold_in(key, 7))
    bounds = jnp.cumsum(sizes)
    starts = bounds - sizes
    blocks_all = jnp.arange(NBLK, dtype=jnp.int32)
    owner = jnp.sum((bounds[None, :] <= blocks_all[:, None]).astype(jnp.int32), axis=1)
    first_block = starts[owner]
    span_blocks = sizes[owner]
    total_rows = NBLK * BLOCK
    row_block = jnp.arange(total_rows, dtype=jnp.int32) // BLOCK
    jumps = jax.random.randint(jax.random.fold_in(key, 31), (total_rows,), 0, MAXB * BLOCK)
    partner_block = first_block[row_block] + jumps // BLOCK % span_blocks[row_block]
    partner_row = partner_block * BLOCK + jumps % BLOCK
    weight_dup = jax.random.uniform(jax.random.fold_in(key, 33), (total_rows, 1), jnp.float32, 0.3, 2.0)
    base = jnp.clip(jax.random.normal(jax.random.fold_in(key, 32), (total_rows, D), jnp.float32), -6.0, 6.0)
    mixed = base + weight_dup * base[partner_row]
    return mixed.astype(jnp.bfloat16)


def setup_inputs(seed: int = 0) -> dict:
    key_list = jax.random.split(jax.random.key(seed), 3)
    embeddings = draw_embeddings(jax.random.fold_in(key_list[2], 71), 0)
    cluster_blocks = draw_cluster_blocks(jax.random.fold_in(key_list[2], 71), 0)
    return {"embeddings": embeddings, "cluster_blocks": cluster_blocks}


EPSILON = 1e-06

def unit_rows(block_rows):
    values = block_rows.astype(jnp.float32)
    scaled = values * lax.rsqrt(lax.optimization_barrier(jnp.sum(values * values, axis=1, keepdims=True)) + EPSILON)
    return scaled.astype(jnp.bfloat16)

def reference(embeddings, cluster_blocks):
    blocks_all = embeddings.shape[0] // BLOCK
    normed = unit_rows(embeddings).astype(jnp.float32).reshape(blocks_all, BLOCK, D)
    bounds = jnp.cumsum(cluster_blocks).astype(jnp.int32)
    positions = jnp.arange(blocks_all, dtype=jnp.int32)
    diagonal_mask = jnp.arange(BLOCK)[:, None] == jnp.arange(BLOCK)[None, :]
    highest = jnp.full((blocks_all, BLOCK), -2.0, jnp.float32)
    for offset in range(MAXB):
        if offset == 0:
            partner = normed
        else:
            partner = jnp.concatenate([jnp.zeros((offset, BLOCK, D), jnp.float32), normed[:-offset]], axis=0)
        lower = positions - offset
        crossing = lax.optimization_barrier(jnp.sum(((bounds[None, :] > lower[:, None]) & (bounds[None, :] <= positions[:, None])).astype(jnp.int32), axis=1))
        allowed = (lower >= 0) & (crossing == 0)

        def tile(items):
            mine, theirs, permitted = items
            products = jnp.dot(mine, theirs.T, precision=lax.Precision.HIGHEST)
            products = jnp.where(permitted, products, -2.0)
            if offset == 0:
                products = jnp.where(diagonal_mask, -2.0, products)
            return (lax.optimization_barrier(jnp.max(products, axis=1)), lax.optimization_barrier(jnp.max(products, axis=0)))
        row_part, col_part = lax.map(tile, (normed, partner, allowed))
        highest = jnp.maximum(highest, row_part)
        if offset > 0:
            returned = jnp.concatenate([col_part[offset:], jnp.full((offset, BLOCK), -2.0, jnp.float32)], axis=0)
            highest = jnp.maximum(highest, returned)
    return highest.reshape(-1)
```

```python
import functools

import jax
import jax.numpy as jnp
from jax import lax
from jax.experimental import pallas as pl
from jax.experimental.pallas import tpu as pltpu
from jax.sharding import PartitionSpec as P

EPSILON = 1e-06
LOW = -2.0
MESH_ID = pl.DeviceIdType.MESH
PIECES = 8
HALF = PIECES // 2
GROUP = 8

NEAR = ((0, 1), (0, 2), (0, 3), (0, 5), (0, 6), (0, 7), (1, 2), (1, 4), (2, 3), (2, 4), (2, 6),
        (3, 5), (3, 6), (4, 5), (4, 6), (5, 6), (5, 7), (6, 7))
ACROSS = ((0, 0), (0, 1), (5, 0), (5, 1), (5, 4), (7, 1), (7, 2), (7, 6))
MAIN_OFFSET = (-8, 1, -2, 3, 2, -5, -1, 7)
MAIN_SLOT = (2, 0, 0, 1, 0, 1, 0, 2)
FIRST_SEEN, LAST_SEEN = -1, 9


def nearest_kernel(sizes, counts_hbm, x_ref, out_ref, raw, own, other, wide_in, stage, acc, *rest):
    rest = list(rest)

    def several(many):
        return [rest.pop(0) for _ in range(many)]

    main_in, half_in, ret_in, lines = several(3), several(2), several(5), [None] + several(6)
    main_recv, half_recv, side_send = several(3), several(2), several(3)
    (load_sem, pair_send, pair_recv, main_send, wide_recv, ret_send, ret_recv,
     counts_ref, counts_sem) = rest
    n_rows, n_bal = sizes
    total = n_rows * n_bal
    block, width = x_ref.shape
    piece = block // PIECES
    tile = 2 * piece
    half = block // 2
    me = lax.axis_index("rows") * n_bal + lax.axis_index("bal")
    role = lax.rem(me, GROUP)
    base = me - role
    has_up = base + GROUP < total
    has_down = base > 0
    partner = me + 1 - 2 * lax.rem(me, 2)

    def coords(index):
        return (index // n_bal, lax.rem(index, n_bal))

    def by_role(values):
        return sum((role == place).astype(jnp.int32) * value for place, value in enumerate(values))

    barrier = pltpu.get_barrier_semaphore()
    near_of = [[b if a == r else a for a, b in NEAR if r in (a, b)] for r in range(GROUP)]
    up_of = [[b for a, b in ACROSS if a == r] for r in range(GROUP)]
    down_of = [[a for a, b in ACROSS if b == r] for r in range(GROUP)]

    def greet(index):
        pl.semaphore_signal(barrier, inc=1, device_id=coords(index), device_id_type=MESH_ID)

    for r in range(GROUP):
        @pl.when(role == r)
        def _():
            @pl.when(has_up)
            def _():
                for there in up_of[r]:
                    greet(me + GROUP + there - r)

            @pl.when(has_down)
            def _():
                for there in down_of[r]:
                    greet(me - GROUP + there - r)

            for there in near_of[r]:
                greet(me + there - r)

    greeted = (by_role([len(n) for n in near_of])
               + has_up.astype(jnp.int32) * by_role([len(n) for n in up_of])
               + has_down.astype(jnp.int32) * by_role([len(n) for n in down_of]))

    def rows_of(q, size=piece):
        return pl.ds(pl.multiple_of(q * size, size), size)

    def load(q):
        return pltpu.make_async_copy(x_ref.at[rows_of(q)], raw.at[rows_of(q)], load_sem.at[q])

    counts_load = pltpu.make_async_copy(counts_hbm, counts_ref, counts_sem)
    counts_load.start()

    @pl.loop(0, PIECES)
    def _(q):
        load(q).start()

    def copy_to(src, dst, send, recv, index):
        return pltpu.make_async_remote_copy(
            src_ref=src, dst_ref=dst, send_sem=send, recv_sem=recv,
            device_id=coords(index), device_id_type=MESH_ID)

    def to_main(r, q):
        slot = MAIN_SLOT[r]
        return copy_to(own.at[rows_of(q)], main_in[slot].at[rows_of(q)],
                       main_send.at[q], main_recv[slot].at[q], me + MAIN_OFFSET[r])

    def for_main(act):
        for r in range(GROUP):
            here = role == r
            if r == 0:
                here = here & has_down
            if r == 7:
                here = here & has_up
            pl.when(here)(functools.partial(act, r))

    def to_pair(q):
        return copy_to(own.at[rows_of(q)], other.at[rows_of(q)], pair_send.at[q], pair_recv.at[q], partner)

    def side(slot, q, src, dst, recv, index):
        return copy_to(src, dst, side_send[slot].at[q], recv, index)

    def high_half(q):
        low = q - HALF
        return side(0, low, own.at[rows_of(q)], half_in[0].at[rows_of(low)], half_recv[0].at[low], me - 7)

    def normalise(q):
        rows = rows_of(q)
        load(q).wait()
        values = raw[rows, :].astype(jnp.float32)
        scale = lax.rsqrt(jnp.sum(values * values, axis=1, keepdims=True) + EPSILON)
        own[rows, :] = (values * scale).astype(jnp.bfloat16)

    def send(q):
        for_main(lambda r: to_main(r, q).start())

        @pl.when((role == 7) & (q >= HALF))
        def _():
            high_half(q).start()

        to_pair(q).start()

    pl.loop(0, HALF)(normalise)
    pl.semaphore_wait(barrier, greeted)
    pl.loop(0, HALF)(send)

    @pl.loop(HALF, PIECES)
    def _(q):
        normalise(q)
        send(q)

    counts_load.wait()

    def count(i, carry):
        end, owners = carry
        end = end + counts_ref[i]
        return end, tuple(
            owner + (end <= base + place).astype(jnp.int32)
            for place, owner in zip(range(FIRST_SEEN, LAST_SEEN + 1), owners))

    zero = jnp.int32(0)
    _, owners = lax.fori_loop(0, counts_ref.shape[0], count,
                              (zero, (zero,) * (LAST_SEEN + 1 - FIRST_SEEN)))

    def same(i, j):
        return owners[i - FIRST_SEEN] == owners[j - FIRST_SEEN]

    whole = same(0, 3)
    below = same(-1, 2) & has_down
    acc[...] = jnp.full(acc.shape, LOW, jnp.float32)

    def products(left, right):
        return lax.dot_general(left, right, (((1,), (1,)), ((), ())),
                               preferred_element_type=jnp.float32)

    def lanes_max(values):
        highest = values[:, :128]
        for start in range(128, values.shape[1], 128):
            highest = jnp.maximum(highest, values[:, start:start + 128])
        return highest

    def raise_to(slot, lanes, top):
        acc[slot, :, lanes] = jnp.maximum(acc[slot, :, lanes], top)

    everywhere = slice(None)
    low_lanes = slice(0, half)
    high_lanes = slice(half, block)

    def meet(left, partners, row_slot, p, shift=0):
        part = None
        for right, permitted, column_slot, lanes in partners:
            values = products(left, right)
            top = jnp.max(values, axis=0, keepdims=True)
            raise_to(column_slot, lanes, jnp.where(permitted, top, LOW))
            across = jnp.where(permitted, lanes_max(values), LOW)
            part = across if part is None else jnp.maximum(part, across)
        lanes = pl.ds(pl.multiple_of(p * tile + shift, tile), tile)
        raise_to(row_slot, lanes, jnp.max(part.T, axis=0, keepdims=True))

    def diagonal():
        @pl.loop(0, block // tile)
        def _(p):
            values = products(own[rows_of(p, tile), :], own[...])
            across = lax.broadcasted_iota(jnp.int32, values.shape, 1)
            down = lax.broadcasted_iota(jnp.int32, values.shape, 0) + p * tile
            values = jnp.where(across == down, LOW, values)
            raise_to(0, everywhere, jnp.max(values, axis=0, keepdims=True))

    def pair_tile(permitted):
        @pl.loop(0, block // tile)
        def _(p):
            meet(other[rows_of(p, tile), :], [(own[...], permitted, 0, everywhere)], 1, p)

    def wait_pair(begin=0, end=PIECES):
        @pl.loop(begin, end)
        def _(q):
            to_pair(q).wait_recv()

    def wait_main(slot, q):
        copy_to(own.at[rows_of(q)], main_in[slot].at[rows_of(q)],
                main_send.at[q], main_recv[slot].at[q], me).wait_recv()

    def wait_wide(q):
        side(0, q, stage.at[rows_of(q)], wide_in.at[rows_of(q)], wide_recv.at[q], me).wait_recv()

    def wait_half(slot, q):
        side(0, q, stage.at[rows_of(q)], half_in[slot].at[rows_of(q)], half_recv[slot].at[q], me).wait_recv()

    def both(wait, p):
        wait(2 * p)
        wait(2 * p + 1)

    def ret(slot, offset, place):
        return copy_to(lines[max(slot, 1)], ret_in[place], ret_send.at[slot], ret_recv.at[place], me + offset)

    def give(slot, offset, place):
        lines[slot][...] = acc[slot]
        ret(slot, offset, place).start()

    tiles = block // tile
    half_tiles = half // tile

    def split(slot, chosen, first_slot, first_lanes, second_slot, second_lanes, lanes):
        acc[first_slot, :, first_lanes] = jnp.where(chosen, acc[slot, :, lanes], LOW)
        acc[second_slot, :, second_lanes] = jnp.where(chosen, LOW, acc[slot, :, lanes])

    def zero_side(q):
        return side(0, q, stage.at[rows_of(q)], half_in[0].at[rows_of(q)], half_recv[0].at[q], me + 3)

    def zero_relay(q):
        return side(1, q, main_in[2].at[rows_of(q)], wide_in.at[rows_of(q)], wide_recv.at[q], me + 5)

    def zero_down(q):
        return side(2, q, other.at[rows_of(q + HALF)], half_in[1].at[rows_of(q)], half_recv[1].at[q], me - 8)

    @pl.when(role == 0)
    def _():
        wait_pair()

        @pl.when(has_down)
        def _():
            @pl.loop(0, HALF)
            def _(q):
                zero_down(q).start()

        diagonal()

        def pass_on(q):
            @pl.when(has_up)
            def _():
                wait_main(2, q)
                zero_relay(q).start()

        @pl.loop(0, HALF)
        def _(q):
            rows = rows_of(q)
            wait_main(1, q)
            stage[rows, :] = jnp.where(whole, own[rows_of(q + HALF), :], main_in[1][rows, :])
            zero_side(q).start()
            pass_on(q)

        @pl.loop(HALF, PIECES)
        def _(q):
            wait_main(1, q)
            pass_on(q)

        @pl.loop(0, half_tiles)
        def _(p):
            both(lambda q: wait_half(0, q), p)
            left = half_in[0][rows_of(p, tile), :]
            meet(left, [(main_in[1][...], same(5, 7), 2, everywhere)], 3, p, half)

            @pl.when(has_up)
            def _():
                meet(left, [(main_in[2][...], same(7, 8), 4, everywhere)], 3, p, half)

        @pl.loop(0, tiles)
        def _(p):
            both(lambda q: wait_main(0, q), p)
            meet(main_in[0][rows_of(p, tile), :],
                 [(own[...], same(0, 2), 0, everywhere), (main_in[1][...], same(2, 5), 2, everywhere)], 1, p)

        give(1, 2, 0)
        give(2, 5, 1)

        @pl.when(has_up)
        def _():
            @pl.loop(0, half_tiles)
            def _(p):
                both(lambda q: wait_half(1, q), p)
                meet(half_in[1][rows_of(p, tile), :], [(half_in[0][...], same(7, 9), 3, high_lanes)], 5, p, half)

            give(4, 8, 4)
            give(5, 9, 2)

        give(3, 7, 2)

    def one_side(q):
        return side(0, q, stage.at[rows_of(q)], half_in[0].at[rows_of(q)], half_recv[0].at[q], me + 3)

    @pl.when(role == 1)
    def _():
        @pl.loop(0, HALF)
        def _(q):
            to_pair(q).wait_recv()
            rows = rows_of(q)
            stage[rows, :] = jnp.where(whole, other[rows, :], own[rows_of(q + HALF), :])
            one_side(q).start()

        diagonal()
        wait_pair(HALF, PIECES)
        pair_tile(same(0, 1))
        give(1, -1, 0)

    def two_down(q):
        return side(0, q, main_in[0].at[rows_of(q)], half_in[0].at[rows_of(q)], half_recv[0].at[q], me - 3)

    @pl.when(role == 2)
    def _():
        wait_pair()
        diagonal()
        from_four = same(1, 4) & jnp.logical_not(below)

        @pl.loop(0, HALF)
        def _(q):
            wait_main(0, q)

            @pl.when(has_down)
            def _():
                two_down(q).start()

        def first_block(p):
            meet(main_in[0][rows_of(p, tile), :],
                 [(own[...], same(1, 2), 0, everywhere), (other[...], same(1, 3), 2, everywhere)], 1, p)

        pl.loop(0, half_tiles)(first_block)

        def chosen_block(p):
            both(wait_wide, p)
            meet(wide_in[rows_of(p, tile), :],
                 [(own[...], below | same(2, 4), 0, everywhere),
                  (main_in[0][:half, :], from_four, 1, low_lanes)], 3, p)

        pl.loop(0, half_tiles)(chosen_block)

        @pl.loop(half_tiles, tiles)
        def _(p):
            both(lambda q: wait_main(0, q), p)
            first_block(p)

        give(2, 1, 0)
        pl.loop(half_tiles, tiles)(chosen_block)

        @pl.loop(half_tiles, tiles)
        def _(p):
            meet(main_in[0][rows_of(p, tile), :], [(wide_in[...], from_four, 3, everywhere)], 1, p)

        split(3, below, 5, everywhere, 4, everywhere, everywhere)
        give(1, -1, 0)
        give(4, 2, 1)

        @pl.when(has_down)
        def _():
            give(5, -3, 3)

    @pl.when(role == 3)
    def _():
        wait_pair()
        diagonal()
        pair_tile(same(2, 3))
        give(1, -1, 1)

        @pl.loop(0, half_tiles)
        def _(p):
            both(lambda q: wait_half(0, q), p)
            meet(half_in[0][rows_of(p, tile), :], [(own[...], whole | same(3, 5), 0, everywhere)], 2, p)

        split(2, whole, 3, high_lanes, 4, low_lanes, low_lanes)
        give(3, -3, 1)
        give(4, 2, 2)

    def four_side(q):
        return side(0, q, stage.at[rows_of(q)], half_in[0].at[rows_of(q)], half_recv[0].at[q], me + 2)

    def four_down(q):
        return side(1, q, half_in[0].at[rows_of(q)], half_in[1].at[rows_of(q)], half_recv[1].at[q], me - 7)

    @pl.when(role == 4)
    def _():
        wait_pair()
        diagonal()

        @pl.loop(0, HALF)
        def _(q):
            wait_half(0, q)

            @pl.when(has_down)
            def _():
                four_down(q).start()

            rows = rows_of(q)
            stage[rows, :] = jnp.where(whole, half_in[0][rows, :], other[rows_of(q + HALF), :])
            four_side(q).start()

        pair_tile(same(4, 5))
        give(1, 1, 0)

    @pl.when(role == 5)
    def _():
        wait_pair()
        diagonal()

        @pl.loop(0, tiles)
        def _(p):
            both(lambda q: wait_main(0, q), p)
            meet(main_in[0][rows_of(p, tile), :], [(own[...], same(5, 6), 0, everywhere)], 1, p)

        @pl.when(has_up)
        def _():
            @pl.loop(0, half_tiles)
            def _(p):
                both(lambda q: wait_half(1, q), p)
                meet(half_in[1][rows_of(p, tile), :], [(main_in[0][...], same(6, 9), 1, everywhere)], 4, p, half)

        @pl.loop(0, half_tiles)
        def _(p):
            @pl.when(has_up)
            def _():
                @pl.loop(2 * p, 2 * p + 2)
                def _(i):
                    both(wait_wide, i)
                    meet(wide_in[rows_of(i, tile), :],
                         [(own[...], same(5, 8), 0, everywhere), (main_in[0][...], same(6, 8), 1, everywhere)], 3, i)

            both(lambda q: wait_half(0, q), p)
            left = half_in[0][rows_of(p, tile), :]
            meet(left, [(own[...], same(5, 7), 0, everywhere)], 2, p)

            @pl.when(has_up)
            def _():
                meet(left, [(half_in[1][...], same(7, 9), 4, high_lanes)], 2, p)

        give(1, 1, 0)

        @pl.when(has_up)
        def _():
            @pl.loop(0, half_tiles)
            def _(p):
                meet(half_in[0][rows_of(p, tile), :], [(wide_in[...], same(7, 8), 3, everywhere)], 2, p)

            give(3, 3, 3)
            give(4, 4, 1)

        give(2, 2, 1)

    def six_side(q):
        return side(0, q, stage.at[rows_of(q)], wide_in.at[rows_of(q)], wide_recv.at[q], me - 4)

    def six_low(q):
        return side(1, q, other.at[rows_of(q)], half_in[0].at[rows_of(q)], half_recv[0].at[q], me - 1)

    @pl.when(role == 6)
    def _():
        wait_pair()

        @pl.loop(0, HALF)
        def _(q):
            six_low(q).start()

        diagonal()

        def choose(q):
            rows = rows_of(q)
            wait_main(0, q)

            @pl.when(has_down)
            def _():
                wait_main(2, q)
                stage[rows, :] = jnp.where(below, main_in[2][rows, :], main_in[0][rows, :])

            @pl.when(jnp.logical_not(has_down))
            def _():
                stage[rows, :] = main_in[0][rows, :]

            six_side(q).start()

        @pl.loop(0, tiles)
        def _(p):
            both(choose, p)
            meet(main_in[0][rows_of(p, tile), :],
                 [(own[...], same(4, 6), 0, everywhere), (other[...], same(4, 7), 2, everywhere)], 1, p)

        give(2, 1, 0)

        @pl.loop(0, tiles)
        def _(p):
            both(lambda q: wait_main(1, q), p)
            meet(main_in[1][rows_of(p, tile), :],
                 [(own[...], same(3, 6), 0, everywhere), (main_in[0][...], same(3, 4), 1, everywhere)], 3, p)

        give(1, -2, 0)

        @pl.loop(0, half_tiles)
        def _(p):
            both(lambda q: wait_half(0, q), p)
            meet(half_in[0][rows_of(p, tile), :], [(main_in[1][...], whole | same(3, 5), 3, everywhere)], 4, p)

        split(4, whole, 5, low_lanes, 6, high_lanes, low_lanes)
        give(3, -3, 1)
        give(5, -6, 2)
        give(6, -1, 3)

    @pl.when(role == 7)
    def _():
        wait_pair()
        diagonal()
        pair_tile(same(6, 7))

        @pl.when(has_up)
        def _():
            @pl.loop(0, half_tiles)
            def _(p):
                both(lambda q: wait_half(0, q), p)
                meet(half_in[0][rows_of(p, tile), :],
                     [(own[...], same(7, 9), 0, everywhere), (other[...], same(6, 9), 1, everywhere)], 2, p)

            give(2, 2, 3)

        give(1, -1, 1)

    def take(*places):
        for place in places:
            ret(0, 0, place).wait_recv()
            raise_to(0, everywhere, ret_in[place][...])

    expected = ((0, 1, 2), (0,), (0, 1), (0, 1), (0, 1), (0, 1, 2, 3), (0, 1), (0, 1, 2))
    for r in range(GROUP):
        @pl.when(role == r)
        def _():
            take(*expected[r])

    @pl.when(has_down & (role == 0))
    def _():
        take(3, 4)

    @pl.when(has_down & (role == 1))
    def _():
        take(1, 2, 3)

    @pl.when(has_up & (role == 7))
    def _():
        take(3)

    out_ref[...] = acc[0]

    @pl.loop(0, PIECES)
    def _(q):
        to_pair(q).wait_send()

        for_main(lambda r: to_main(r, q).wait_send())

        @pl.when((role == 0) & has_up)
        def _():
            zero_relay(q).wait_send()

        @pl.when(role == 6)
        def _():
            six_side(q).wait_send()

    @pl.loop(0, HALF)
    def _(q):
        @pl.when(role == 0)
        def _():
            zero_side(q).wait_send()

            @pl.when(has_down)
            def _():
                zero_down(q).wait_send()

        @pl.when(role == 1)
        def _():
            one_side(q).wait_send()

        @pl.when((role == 2) & has_down)
        def _():
            two_down(q).wait_send()

        @pl.when(role == 4)
        def _():
            four_side(q).wait_send()

            @pl.when(has_down)
            def _():
                four_down(q).wait_send()

        @pl.when(role == 6)
        def _():
            six_low(q).wait_send()

        @pl.when(role == 7)
        def _():
            high_half(q + HALF).wait_send()

    sent = ((1, 2, 3), (1,), (1, 2, 4), (1, 3, 4), (1,), (1, 2), (1, 2, 3, 5, 6), (1,))
    sent_up = ((4, 5), (), (), (), (), (3, 4), (), (2,))
    for r in range(GROUP):
        @pl.when(role == r)
        def _():
            for slot in sent[r]:
                ret(slot, 0, 0).wait_send()

            @pl.when(has_up)
            def _():
                for slot in sent_up[r]:
                    ret(slot, 0, 0).wait_send()

    @pl.when((role == 2) & has_down)
    def _():
        ret(5, 0, 0).wait_send()


def shards(sizes, embeddings, cluster_blocks):
    block, width = embeddings.shape
    wide = pltpu.VMEM((block, width), jnp.bfloat16)
    half = pltpu.VMEM((block // 2, width), jnp.bfloat16)
    line = pltpu.VMEM((1, block), jnp.float32)
    flags = pltpu.SemaphoreType.DMA((PIECES,))
    lone = pltpu.SemaphoreType.DMA
    out = pl.pallas_call(
        functools.partial(nearest_kernel, sizes),
        out_shape=pltpu.VMEM((1, block), jnp.float32),
        in_specs=[pl.BlockSpec(memory_space=pl.ANY)] * 2,
        out_specs=pl.BlockSpec(memory_space=pltpu.VMEM),
        scratch_shapes=[
            wide, wide, wide, wide, wide,
            pltpu.VMEM((8, 1, block), jnp.float32),
            wide, wide, wide, half, half, *[line] * 11, *[flags] * 8,
            flags, flags, flags, flags, flags,
            pltpu.SemaphoreType.DMA((7,)), pltpu.SemaphoreType.DMA((5,)),
            pltpu.SMEM(cluster_blocks.shape, jnp.int32), lone,
        ],
        compiler_params=pltpu.CompilerParams(collective_id=0, has_side_effects=True),
        name="nearest",
    )(cluster_blocks, embeddings)
    return out.reshape(-1)


def solution(mesh):
    sizes = (mesh.shape["rows"], mesh.shape["bal"])
    return jax.shard_map(
        functools.partial(shards, sizes), mesh=mesh,
        in_specs=(P(("rows", "bal"), None), P()), out_specs=P(("rows", "bal")), check_vma=False)
```

```python
import functools

import jax
import jax.numpy as jnp
from jax import lax
from jax.experimental import pallas as pl
from jax.experimental.pallas import tpu as pltpu
from jax.sharding import PartitionSpec as P

EPSILON = 1e-06
LOW = -2.0
MESH_ID = pl.DeviceIdType.MESH
PIECES = 8
HALF = PIECES // 2
GROUP = 8

NEAR = ((0, 1), (1, 0), (2, 3), (3, 2), (4, 5), (5, 4), (6, 7), (7, 6),
        (0, 2), (0, 5), (0, 7), (2, 1), (2, 6), (3, 0), (4, 1), (5, 6), (6, 3), (6, 4))
UPWARD = ((0, 0), (5, 4))
DOWNWARD = ((6, 7),)
MAIN_OFFSET = (-8, 1, -2, 3, 2, -5, -1, 7)
MAIN_SLOT = (2, 0, 0, 1, 0, 1, 0, 2)
FIRST_SEEN, LAST_SEEN = -1, 9


def nearest_kernel(sizes, counts_hbm, x_ref, out_ref, raw, own, other, wide_in, stage, acc, *rest):
    rest = list(rest)

    def several(many):
        return [rest.pop(0) for _ in range(many)]

    main_in, half_in, ret_in, lines = several(3), several(2), several(5), [None] + several(6)
    main_recv, half_recv, side_send = several(3), several(2), several(3)
    (load_sem, pair_send, pair_recv, main_send, wide_recv, ret_send, ret_recv,
     counts_ref, counts_sem) = rest
    n_rows, n_bal = sizes
    total = n_rows * n_bal
    block, width = x_ref.shape
    piece = block // PIECES
    tile = 2 * piece
    half = block // 2
    me = lax.axis_index("rows") * n_bal + lax.axis_index("bal")
    role = lax.rem(me, GROUP)
    base = me - role
    has_up = base + GROUP < total
    has_down = base > 0
    partner = me + 1 - 2 * lax.rem(me, 2)

    def coords(index):
        return (index // n_bal, lax.rem(index, n_bal))

    def by_role(values):
        return sum((role == place).astype(jnp.int32) * value for place, value in enumerate(values))

    barrier = pltpu.get_barrier_semaphore()
    def told_by(edges, r):
        return [there for here, there in edges if here == r]

    def heard_by(edges):
        return by_role([sum(there == r for _, there in edges) for r in range(GROUP)])

    def greet(index):
        pl.semaphore_signal(barrier, inc=1, device_id=coords(index), device_id_type=MESH_ID)

    for r in range(GROUP):
        @pl.when(role == r)
        def _():
            for there in told_by(NEAR, r):
                greet(me + there - r)

            for edges, exists, step in ((UPWARD, has_up, GROUP), (DOWNWARD, has_down, -GROUP)):
                if told_by(edges, r):
                    @pl.when(exists)
                    def _():
                        for there in told_by(edges, r):
                            greet(me + step + there - r)

    greeted = (heard_by(NEAR) + has_down.astype(jnp.int32) * heard_by(UPWARD)
               + has_up.astype(jnp.int32) * heard_by(DOWNWARD))

    def rows_of(q, size=piece):
        return pl.ds(pl.multiple_of(q * size, size), size)

    def load(q):
        return pltpu.make_async_copy(x_ref.at[rows_of(q)], raw.at[rows_of(q)], load_sem.at[q])

    counts_load = pltpu.make_async_copy(counts_hbm, counts_ref, counts_sem)
    counts_load.start()

    @pl.loop(0, PIECES)
    def _(q):
        load(q).start()

    def copy_to(src, dst, send, recv, index):
        return pltpu.make_async_remote_copy(
            src_ref=src, dst_ref=dst, send_sem=send, recv_sem=recv,
            device_id=coords(index), device_id_type=MESH_ID)

    def to_main(r, q):
        slot = MAIN_SLOT[r]
        return copy_to(own.at[rows_of(q)], main_in[slot].at[rows_of(q)],
                       main_send.at[q], main_recv[slot].at[q], me + MAIN_OFFSET[r])

    def for_main(act):
        for r in range(GROUP):
            here = role == r
            if r == 0:
                here = here & has_down
            if r == 7:
                here = here & has_up
            pl.when(here)(functools.partial(act, r))

    def to_pair(q):
        return copy_to(own.at[rows_of(q)], other.at[rows_of(q)], pair_send.at[q], pair_recv.at[q], partner)

    def side(slot, q, src, dst, recv, index):
        return copy_to(src, dst, side_send[slot].at[q], recv, index)

    def high_half(q):
        low = q - HALF
        return side(0, low, own.at[rows_of(q)], half_in[0].at[rows_of(low)], half_recv[0].at[low], me - 7)

    def normalise(q):
        rows = rows_of(q)
        load(q).wait()
        values = raw[rows, :].astype(jnp.float32)
        scale = lax.rsqrt(jnp.sum(values * values, axis=1, keepdims=True) + EPSILON)
        own[rows, :] = (values * scale).astype(jnp.bfloat16)

    def send(q):
        for_main(lambda r: to_main(r, q).start())

        @pl.when((role == 7) & (q >= HALF))
        def _():
            high_half(q).start()

        to_pair(q).start()

    pl.loop(0, HALF)(normalise)
    pl.semaphore_wait(barrier, greeted)
    pl.loop(0, HALF)(send)

    @pl.loop(HALF, PIECES)
    def _(q):
        normalise(q)
        send(q)

    counts_load.wait()

    def count(i, carry):
        end, owners = carry
        end = end + counts_ref[i]
        return end, tuple(
            owner + (end <= base + place).astype(jnp.int32)
            for place, owner in zip(range(FIRST_SEEN, LAST_SEEN + 1), owners))

    zero = jnp.int32(0)
    _, owners = lax.fori_loop(0, counts_ref.shape[0], count,
                              (zero, (zero,) * (LAST_SEEN + 1 - FIRST_SEEN)))

    def same(i, j):
        return owners[i - FIRST_SEEN] == owners[j - FIRST_SEEN]

    whole = same(0, 3)
    below = same(-1, 2) & has_down
    acc[...] = jnp.full(acc.shape, LOW, jnp.float32)

    def products(left, right):
        return lax.dot_general(left, right, (((1,), (1,)), ((), ())),
                               preferred_element_type=jnp.float32)

    def lanes_max(values):
        highest = values[:, :128]
        for start in range(128, values.shape[1], 128):
            highest = jnp.maximum(highest, values[:, start:start + 128])
        return highest

    def raise_to(slot, lanes, top):
        acc[slot, :, lanes] = jnp.maximum(acc[slot, :, lanes], top)

    everywhere = slice(None)
    low_lanes = slice(0, half)
    high_lanes = slice(half, block)

    def meet(left, partners, row_slot, p, shift=0):
        part = None
        for right, permitted, column_slot, lanes in partners:
            values = products(left, right)
            top = jnp.max(values, axis=0, keepdims=True)
            raise_to(column_slot, lanes, jnp.where(permitted, top, LOW))
            across = jnp.where(permitted, lanes_max(values), LOW)
            part = across if part is None else jnp.maximum(part, across)
        lanes = pl.ds(pl.multiple_of(p * tile + shift, tile), tile)
        raise_to(row_slot, lanes, jnp.max(part.T, axis=0, keepdims=True))

    def diagonal():
        @pl.loop(0, block // tile)
        def _(p):
            values = products(own[rows_of(p, tile), :], own[...])
            across = lax.broadcasted_iota(jnp.int32, values.shape, 1)
            down = lax.broadcasted_iota(jnp.int32, values.shape, 0) + p * tile
            values = jnp.where(across == down, LOW, values)
            raise_to(0, everywhere, jnp.max(values, axis=0, keepdims=True))

    def pair_tile(permitted):
        @pl.loop(0, block // tile)
        def _(p):
            meet(other[rows_of(p, tile), :], [(own[...], permitted, 0, everywhere)], 1, p)

    def wait_pair(begin=0, end=PIECES):
        @pl.loop(begin, end)
        def _(q):
            to_pair(q).wait_recv()

    def wait_main(slot, q):
        copy_to(own.at[rows_of(q)], main_in[slot].at[rows_of(q)],
                main_send.at[q], main_recv[slot].at[q], me).wait_recv()

    def wait_wide(q):
        side(0, q, stage.at[rows_of(q)], wide_in.at[rows_of(q)], wide_recv.at[q], me).wait_recv()

    def wait_half(slot, q):
        side(0, q, stage.at[rows_of(q)], half_in[slot].at[rows_of(q)], half_recv[slot].at[q], me).wait_recv()

    def both(wait, p):
        wait(2 * p)
        wait(2 * p + 1)

    def ret(slot, offset, place):
        return copy_to(lines[max(slot, 1)], ret_in[place], ret_send.at[slot], ret_recv.at[place], me + offset)

    def give(slot, offset, place):
        lines[slot][...] = acc[slot]
        ret(slot, offset, place).start()

    tiles = block // tile
    half_tiles = half // tile

    def split(slot, chosen, first_slot, first_lanes, second_slot, second_lanes, lanes):
        acc[first_slot, :, first_lanes] = jnp.where(chosen, acc[slot, :, lanes], LOW)
        acc[second_slot, :, second_lanes] = jnp.where(chosen, LOW, acc[slot, :, lanes])

    def zero_side(q):
        return side(0, q, stage.at[rows_of(q)], half_in[0].at[rows_of(q)], half_recv[0].at[q], me + 3)

    def zero_relay(q):
        return side(1, q, main_in[2].at[rows_of(q)], wide_in.at[rows_of(q)], wide_recv.at[q], me + 5)

    def zero_down(q):
        return side(2, q, other.at[rows_of(q + HALF)], half_in[1].at[rows_of(q)], half_recv[1].at[q], me - 8)

    @pl.when(role == 0)
    def _():
        wait_pair()

        @pl.when(has_down)
        def _():
            @pl.loop(0, HALF)
            def _(q):
                zero_down(q).start()

        diagonal()

        def pass_on(q):
            @pl.when(has_up)
            def _():
                wait_main(2, q)
                zero_relay(q).start()

        @pl.loop(0, HALF)
        def _(q):
            rows = rows_of(q)
            wait_main(1, q)
            stage[rows, :] = jnp.where(whole, own[rows_of(q + HALF), :], main_in[1][rows, :])
            zero_side(q).start()
            pass_on(q)

        @pl.loop(HALF, PIECES)
        def _(q):
            wait_main(1, q)
            pass_on(q)

        @pl.loop(0, half_tiles)
        def _(p):
            both(lambda q: wait_half(0, q), p)
            left = half_in[0][rows_of(p, tile), :]
            meet(left, [(main_in[1][...], same(5, 7), 2, everywhere)], 3, p, half)

            @pl.when(has_up)
            def _():
                meet(left, [(main_in[2][...], same(7, 8), 4, everywhere)], 3, p, half)

        @pl.loop(0, half_tiles)
        def _(j):
            @pl.loop(3 * j, 3 + j)
            def _(p):
                both(lambda q: wait_main(0, q), p)
                meet(main_in[0][rows_of(p, tile), :],
                     [(own[...], same(0, 2), 0, everywhere), (main_in[1][...], same(2, 5), 2, everywhere)], 1, p)

            @pl.when(has_up)
            def _():
                both(lambda q: wait_half(1, q), j)
                meet(half_in[1][rows_of(j, tile), :], [(half_in[0][...], same(7, 9), 3, high_lanes)], 5, j, half)

        give(3, 7, 2)
        give(1, 2, 0)
        give(2, 5, 1)

        @pl.when(has_up)
        def _():
            give(4, 8, 4)
            give(5, 9, 2)

    def one_side(q):
        return side(0, q, stage.at[rows_of(q)], half_in[0].at[rows_of(q)], half_recv[0].at[q], me + 3)

    @pl.when(role == 1)
    def _():
        @pl.loop(0, HALF)
        def _(q):
            to_pair(q).wait_recv()
            rows = rows_of(q)
            stage[rows, :] = jnp.where(whole, other[rows, :], own[rows_of(q + HALF), :])
            one_side(q).start()

        diagonal()
        wait_pair(HALF, PIECES)
        pair_tile(same(0, 1))
        give(1, -1, 0)

    def two_down(q):
        return side(0, q, main_in[0].at[rows_of(q)], half_in[0].at[rows_of(q)], half_recv[0].at[q], me - 3)

    @pl.when(role == 2)
    def _():
        wait_pair()
        diagonal()
        from_four = same(1, 4) & jnp.logical_not(below)

        wait_wide(0)

        @pl.loop(0, HALF)
        def _(q):
            wait_main(0, q)

            @pl.when(has_down)
            def _():
                two_down(q).start()

        def first_block(p):
            meet(main_in[0][rows_of(p, tile), :],
                 [(own[...], same(1, 2), 0, everywhere), (other[...], same(1, 3), 2, everywhere)], 1, p)

        pl.loop(0, half_tiles)(first_block)
        pl.loop(1, HALF)(wait_wide)

        @pl.loop(0, half_tiles)
        def _(p):
            meet(wide_in[rows_of(p, tile), :],
                 [(own[...], below | same(2, 4), 0, everywhere),
                  (main_in[0][:half, :], from_four, 1, low_lanes)], 3, p)

        @pl.loop(half_tiles, tiles)
        def _(p):
            both(lambda q: wait_main(0, q), p)
            meet(main_in[0][rows_of(p, tile), :],
                 [(own[...], same(1, 2), 0, everywhere), (other[...], same(1, 3), 2, everywhere),
                  (wide_in[:half, :], from_four, 3, low_lanes)], 1, p)

        give(2, 1, 0)

        @pl.loop(half_tiles, tiles)
        def _(p):
            both(wait_wide, p)
            meet(wide_in[rows_of(p, tile), :],
                 [(own[...], below | same(2, 4), 0, everywhere),
                  (main_in[0][...], from_four, 1, everywhere)], 3, p)

        split(3, below, 5, everywhere, 4, everywhere, everywhere)
        give(1, -1, 0)
        give(4, 2, 1)

        @pl.when(has_down)
        def _():
            give(5, -3, 3)

    @pl.when(role == 3)
    def _():
        wait_pair()
        diagonal()
        pair_tile(same(2, 3))
        give(1, -1, 1)

        @pl.loop(0, half_tiles)
        def _(p):
            both(lambda q: wait_half(0, q), p)
            meet(half_in[0][rows_of(p, tile), :], [(own[...], whole | same(3, 5), 0, everywhere)], 2, p)

        split(2, whole, 3, high_lanes, 4, low_lanes, low_lanes)
        give(3, -3, 1)
        give(4, 2, 2)

    def four_side(q):
        return side(0, q, stage.at[rows_of(q)], half_in[0].at[rows_of(q)], half_recv[0].at[q], me + 2)

    def four_down(q):
        return side(1, q, half_in[0].at[rows_of(q)], half_in[1].at[rows_of(q)], half_recv[1].at[q], me - 7)

    @pl.when(role == 4)
    def _():
        wait_pair()
        diagonal()

        @pl.loop(0, HALF)
        def _(q):
            wait_half(0, q)

            @pl.when(has_down)
            def _():
                four_down(q).start()

            rows = rows_of(q)
            stage[rows, :] = jnp.where(whole, half_in[0][rows, :], other[rows_of(q + HALF), :])
            four_side(q).start()

        pair_tile(same(4, 5))
        give(1, 1, 0)

    @pl.when(role == 5)
    def _():
        wait_pair()
        diagonal()

        @pl.loop(0, tiles)
        def _(p):
            both(lambda q: wait_main(0, q), p)
            meet(main_in[0][rows_of(p, tile), :], [(own[...], same(5, 6), 0, everywhere)], 1, p)

        @pl.when(has_up)
        def _():
            @pl.loop(0, half_tiles)
            def _(p):
                both(lambda q: wait_half(1, q), p)
                meet(half_in[1][rows_of(p, tile), :], [(main_in[0][...], same(6, 9), 1, everywhere)], 4, p, half)

        @pl.loop(0, half_tiles)
        def _(p):
            @pl.when(has_up)
            def _():
                @pl.loop(2 * p, 2 + p)
                def _(i):
                    both(wait_wide, i)
                    meet(wide_in[rows_of(i, tile), :],
                         [(own[...], same(5, 8), 0, everywhere), (main_in[0][...], same(6, 8), 1, everywhere)], 3, i)

            both(lambda q: wait_half(0, q), p)
            left = half_in[0][rows_of(p, tile), :]
            meet(left, [(own[...], same(5, 7), 0, everywhere)], 2, p)

            @pl.when(has_up)
            def _():
                meet(left, [(half_in[1][...], same(7, 9), 4, high_lanes)], 2, p)

        @pl.when(has_up)
        def _():
            early = block - tile

            @pl.loop(0, half_tiles)
            def _(p):
                meet(half_in[0][rows_of(p, tile), :],
                     [(wide_in[:early, :], same(7, 8), 3, slice(0, early))], 2, p)

            both(wait_wide, tiles - 1)
            meet(wide_in[early:, :],
                 [(own[...], same(5, 8), 0, everywhere), (main_in[0][...], same(6, 8), 1, everywhere),
                  (half_in[0][...], same(7, 8), 2, low_lanes)], 3, tiles - 1)
            give(3, 3, 3)
            give(4, 4, 1)

        give(2, 2, 1)
        give(1, 1, 0)

    def six_side(q):
        return side(0, q, stage.at[rows_of(q)], wide_in.at[rows_of(q)], wide_recv.at[q], me - 4)

    def six_low(q):
        return side(1, q, other.at[rows_of(q)], half_in[0].at[rows_of(q)], half_recv[0].at[q], me - 1)

    @pl.when(role == 6)
    def _():
        wait_pair()

        @pl.loop(0, HALF)
        def _(q):
            six_low(q).start()

        diagonal()

        def choose(q):
            rows = rows_of(q)
            wait_main(0, q)

            @pl.when(has_down)
            def _():
                wait_main(2, q)
                stage[rows, :] = jnp.where(below, main_in[2][rows, :], main_in[0][rows, :])

            @pl.when(jnp.logical_not(has_down))
            def _():
                stage[rows, :] = main_in[0][rows, :]

            six_side(q).start()

        @pl.loop(0, tiles)
        def _(p):
            both(choose, p)
            meet(main_in[0][rows_of(p, tile), :],
                 [(own[...], same(4, 6), 0, everywhere), (other[...], same(4, 7), 2, everywhere)], 1, p)

        give(2, 1, 0)

        @pl.loop(0, tiles)
        def _(p):
            both(lambda q: wait_main(1, q), p)
            meet(main_in[1][rows_of(p, tile), :],
                 [(own[...], same(3, 6), 0, everywhere), (main_in[0][...], same(3, 4), 1, everywhere)], 3, p)

        give(1, -2, 0)

        @pl.loop(0, half_tiles)
        def _(p):
            both(lambda q: wait_half(0, q), p)
            meet(half_in[0][rows_of(p, tile), :], [(main_in[1][...], whole | same(3, 5), 3, everywhere)], 4, p)

        split(4, whole, 5, low_lanes, 6, high_lanes, low_lanes)
        give(3, -3, 1)
        give(5, -6, 2)
        give(6, -1, 3)

    @pl.when(role == 7)
    def _():
        wait_pair()
        diagonal()
        pair_tile(same(6, 7))

        @pl.when(has_up)
        def _():
            @pl.loop(0, half_tiles)
            def _(p):
                both(lambda q: wait_half(0, q), p)
                meet(half_in[0][rows_of(p, tile), :],
                     [(own[...], same(7, 9), 0, everywhere), (other[...], same(6, 9), 1, everywhere)], 2, p)

            give(2, 2, 3)

        give(1, -1, 1)

    def take(*places):
        for place in places:
            ret(0, 0, place).wait_recv()
            raise_to(0, everywhere, ret_in[place][...])

    expected = ((0, 1, 2), (0,), (0, 1), (0, 1), (0, 1), (0, 1, 2, 3), (0, 1), (0, 1, 2))
    for r in range(GROUP):
        @pl.when(role == r)
        def _():
            take(*expected[r])

    @pl.when(has_down & (role == 0))
    def _():
        take(3, 4)

    @pl.when(has_down & (role == 1))
    def _():
        take(1, 2, 3)

    @pl.when(has_up & (role == 7))
    def _():
        take(3)

    out_ref[...] = acc[0]

    @pl.loop(0, PIECES)
    def _(q):
        to_pair(q).wait_send()

        for_main(lambda r: to_main(r, q).wait_send())

        @pl.when((role == 0) & has_up)
        def _():
            zero_relay(q).wait_send()

        @pl.when(role == 6)
        def _():
            six_side(q).wait_send()

    @pl.loop(0, HALF)
    def _(q):
        @pl.when(role == 0)
        def _():
            zero_side(q).wait_send()

            @pl.when(has_down)
            def _():
                zero_down(q).wait_send()

        @pl.when(role == 1)
        def _():
            one_side(q).wait_send()

        @pl.when((role == 2) & has_down)
        def _():
            two_down(q).wait_send()

        @pl.when(role == 4)
        def _():
            four_side(q).wait_send()

            @pl.when(has_down)
            def _():
                four_down(q).wait_send()

        @pl.when(role == 6)
        def _():
            six_low(q).wait_send()

        @pl.when(role == 7)
        def _():
            high_half(q + HALF).wait_send()

    sent = ((1, 2, 3), (1,), (1, 2, 4), (1, 3, 4), (1,), (1, 2), (1, 2, 3, 5, 6), (1,))
    sent_up = ((4, 5), (), (), (), (), (3, 4), (), (2,))
    for r in range(GROUP):
        @pl.when(role == r)
        def _():
            for slot in sent[r]:
                ret(slot, 0, 0).wait_send()

            @pl.when(has_up)
            def _():
                for slot in sent_up[r]:
                    ret(slot, 0, 0).wait_send()

    @pl.when((role == 2) & has_down)
    def _():
        ret(5, 0, 0).wait_send()


def shards(sizes, embeddings, cluster_blocks):
    block, width = embeddings.shape
    wide = pltpu.VMEM((block, width), jnp.bfloat16)
    half = pltpu.VMEM((block // 2, width), jnp.bfloat16)
    line = pltpu.VMEM((1, block), jnp.float32)
    flags = pltpu.SemaphoreType.DMA((PIECES,))
    lone = pltpu.SemaphoreType.DMA
    out = pl.pallas_call(
        functools.partial(nearest_kernel, sizes),
        out_shape=pltpu.VMEM((1, block), jnp.float32),
        in_specs=[pl.BlockSpec(memory_space=pl.ANY)] * 2,
        out_specs=pl.BlockSpec(memory_space=pltpu.VMEM),
        scratch_shapes=[
            wide, wide, wide, wide, wide,
            pltpu.VMEM((8, 1, block), jnp.float32),
            wide, wide, wide, half, half, *[line] * 11, *[flags] * 8,
            flags, flags, flags, flags, flags,
            pltpu.SemaphoreType.DMA((7,)), pltpu.SemaphoreType.DMA((5,)),
            pltpu.SMEM(cluster_blocks.shape, jnp.int32), lone,
        ],
        compiler_params=pltpu.CompilerParams(collective_id=0, has_side_effects=True),
        name="nearest",
    )(cluster_blocks, embeddings)
    return out.reshape(-1)


def solution(mesh):
    sizes = (mesh.shape["rows"], mesh.shape["bal"])
    return jax.shard_map(
        functools.partial(shards, sizes), mesh=mesh,
        in_specs=(P(("rows", "bal"), None), P()), out_specs=P(("rows", "bal")), check_vma=False)
```

```python
import functools

import jax
import jax.numpy as jnp
from jax import lax
from jax.experimental import pallas as pl
from jax.experimental.pallas import tpu as pltpu
from jax.sharding import PartitionSpec as P

EPSILON = 1e-06
LOW = -2.0
MESH_ID = pl.DeviceIdType.MESH
PIECES = 4
HALF = PIECES // 2
GROUP = 8

NEAR = ((0, 1), (1, 0), (2, 3), (3, 2), (4, 5), (5, 4), (6, 7), (7, 6),
        (0, 2), (0, 5), (0, 7), (2, 1), (2, 6), (3, 0), (4, 1), (5, 6), (6, 3), (6, 4))
UPWARD = ((0, 0), (5, 4))
DOWNWARD = ((6, 7),)
MAIN_OFFSET = (-8, 1, -2, 3, 2, -5, -1, 7)
MAIN_SLOT = (2, 0, 0, 1, 0, 1, 0, 2)
FIRST_SEEN, LAST_SEEN = -1, 9


def nearest_kernel(sizes, counts_hbm, x_ref, out_ref, raw, own, other, wide_in, stage, acc, *rest):
    rest = list(rest)

    def several(many):
        return [rest.pop(0) for _ in range(many)]

    main_in, half_in, ret_in, lines = several(3), several(2), several(5), [None] + several(6)
    main_recv, half_recv, side_send = several(3), several(2), several(3)
    (load_sem, pair_send, pair_recv, main_send, wide_recv, ret_send, ret_recv,
     counts_ref, counts_sem) = rest
    n_rows, n_bal = sizes
    total = n_rows * n_bal
    block, width = x_ref.shape
    piece = block // PIECES
    tile = block // 4
    half = block // 2
    me = lax.axis_index("rows") * n_bal + lax.axis_index("bal")
    role = lax.rem(me, GROUP)
    base = me - role
    has_up = base + GROUP < total
    has_down = base > 0
    partner = me + 1 - 2 * lax.rem(me, 2)

    def coords(index):
        return (index // n_bal, lax.rem(index, n_bal))

    def by_role(values):
        return sum((role == place).astype(jnp.int32) * value for place, value in enumerate(values))

    barrier = pltpu.get_barrier_semaphore()
    def told_by(edges, r):
        return [there for here, there in edges if here == r]

    def heard_by(edges):
        return by_role([sum(there == r for _, there in edges) for r in range(GROUP)])

    def greet(index):
        pl.semaphore_signal(barrier, inc=1, device_id=coords(index), device_id_type=MESH_ID)

    for r in range(GROUP):
        @pl.when(role == r)
        def _():
            for there in told_by(NEAR, r):
                greet(me + there - r)

            for edges, exists, step in ((UPWARD, has_up, GROUP), (DOWNWARD, has_down, -GROUP)):
                if told_by(edges, r):
                    @pl.when(exists)
                    def _():
                        for there in told_by(edges, r):
                            greet(me + step + there - r)

    greeted = (heard_by(NEAR) + has_down.astype(jnp.int32) * heard_by(UPWARD)
               + has_up.astype(jnp.int32) * heard_by(DOWNWARD))

    def rows_of(q, size=piece):
        return pl.ds(pl.multiple_of(q * size, size), size)

    def load(q):
        return pltpu.make_async_copy(x_ref.at[rows_of(q)], raw.at[rows_of(q)], load_sem.at[q])

    counts_load = pltpu.make_async_copy(counts_hbm, counts_ref, counts_sem)
    counts_load.start()

    @pl.loop(0, PIECES)
    def _(q):
        load(q).start()

    def copy_to(src, dst, send, recv, index):
        return pltpu.make_async_remote_copy(
            src_ref=src, dst_ref=dst, send_sem=send, recv_sem=recv,
            device_id=coords(index), device_id_type=MESH_ID)

    def to_main(r, q):
        slot = MAIN_SLOT[r]
        return copy_to(own.at[rows_of(q)], main_in[slot].at[rows_of(q)],
                       main_send.at[q], main_recv[slot].at[q], me + MAIN_OFFSET[r])

    def for_main(act):
        for r in range(GROUP):
            here = role == r
            if r == 0:
                here = here & has_down
            if r == 7:
                here = here & has_up
            pl.when(here)(functools.partial(act, r))

    def to_pair(q):
        return copy_to(own.at[rows_of(q)], other.at[rows_of(q)], pair_send.at[q], pair_recv.at[q], partner)

    def side(slot, q, src, dst, recv, index):
        return copy_to(src, dst, side_send[slot].at[q], recv, index)

    def high_half(q):
        low = q - HALF
        return side(0, low, own.at[rows_of(q)], half_in[0].at[rows_of(low)], half_recv[0].at[low], me - 7)

    def normalise(q):
        rows = rows_of(q)
        load(q).wait()
        values = raw[rows, :].astype(jnp.float32)
        scale = lax.rsqrt(jnp.sum(values * values, axis=1, keepdims=True) + EPSILON)
        own[rows, :] = (values * scale).astype(jnp.bfloat16)

    def send(q):
        for_main(lambda r: to_main(r, q).start())

        @pl.when((role == 7) & (q >= HALF))
        def _():
            high_half(q).start()

        to_pair(q).start()

    pl.loop(0, HALF)(normalise)
    pl.semaphore_wait(barrier, greeted)
    pl.loop(0, HALF)(send)

    @pl.loop(HALF, PIECES)
    def _(q):
        normalise(q)
        send(q)

    counts_load.wait()

    def count(i, carry):
        end, owners = carry
        end = end + counts_ref[i]
        return end, tuple(
            owner + (end <= base + place).astype(jnp.int32)
            for place, owner in zip(range(FIRST_SEEN, LAST_SEEN + 1), owners))

    zero = jnp.int32(0)
    _, owners = lax.fori_loop(0, counts_ref.shape[0], count,
                              (zero, (zero,) * (LAST_SEEN + 1 - FIRST_SEEN)))

    def same(i, j):
        return owners[i - FIRST_SEEN] == owners[j - FIRST_SEEN]

    whole = same(0, 3)
    below = same(-1, 2) & has_down
    acc[...] = jnp.full(acc.shape, LOW, jnp.float32)

    def products(left, right):
        return lax.dot_general(left, right, (((1,), (1,)), ((), ())),
                               preferred_element_type=jnp.float32)

    def lanes_max(values):
        highest = values[:, :128]
        for start in range(128, values.shape[1], 128):
            highest = jnp.maximum(highest, values[:, start:start + 128])
        return highest

    def raise_to(slot, lanes, top):
        acc[slot, :, lanes] = jnp.maximum(acc[slot, :, lanes], top)

    everywhere = slice(None)
    low_lanes = slice(0, half)
    high_lanes = slice(half, block)

    def meet(left, partners, row_slot, p, shift=0):
        part = None
        for right, permitted, column_slot, lanes in partners:
            values = products(left, right)
            top = jnp.max(values, axis=0, keepdims=True)
            raise_to(column_slot, lanes, jnp.where(permitted, top, LOW))
            across = jnp.where(permitted, lanes_max(values), LOW)
            part = across if part is None else jnp.maximum(part, across)
        lanes = pl.ds(pl.multiple_of(p * tile + shift, tile), tile)
        raise_to(row_slot, lanes, jnp.max(part.T, axis=0, keepdims=True))

    def diagonal():
        @pl.loop(0, block // tile)
        def _(p):
            values = products(own[rows_of(p, tile), :], own[...])
            across = lax.broadcasted_iota(jnp.int32, values.shape, 1)
            down = lax.broadcasted_iota(jnp.int32, values.shape, 0) + p * tile
            values = jnp.where(across == down, LOW, values)
            raise_to(0, everywhere, jnp.max(values, axis=0, keepdims=True))

    def pair_tile(permitted):
        @pl.loop(0, block // tile)
        def _(p):
            meet(other[rows_of(p, tile), :], [(own[...], permitted, 0, everywhere)], 1, p)

    def wait_pair(begin=0, end=PIECES):
        @pl.loop(begin, end)
        def _(q):
            to_pair(q).wait_recv()

    def wait_main(slot, q):
        copy_to(own.at[rows_of(q)], main_in[slot].at[rows_of(q)],
                main_send.at[q], main_recv[slot].at[q], me).wait_recv()

    def wait_wide(q):
        side(0, q, stage.at[rows_of(q)], wide_in.at[rows_of(q)], wide_recv.at[q], me).wait_recv()

    def wait_half(slot, q):
        side(0, q, stage.at[rows_of(q)], half_in[slot].at[rows_of(q)], half_recv[slot].at[q], me).wait_recv()

    def both(wait, p):
        many = tile // piece
        for k in range(many):
            wait(many * p + k)

    def ret(slot, offset, place):
        return copy_to(lines[max(slot, 1)], ret_in[place], ret_send.at[slot], ret_recv.at[place], me + offset)

    def give(slot, offset, place):
        lines[slot][...] = acc[slot]
        ret(slot, offset, place).start()

    tiles = block // tile
    half_tiles = half // tile

    def split(slot, chosen, first_slot, first_lanes, second_slot, second_lanes, lanes):
        acc[first_slot, :, first_lanes] = jnp.where(chosen, acc[slot, :, lanes], LOW)
        acc[second_slot, :, second_lanes] = jnp.where(chosen, LOW, acc[slot, :, lanes])

    def zero_side(q):
        return side(0, q, stage.at[rows_of(q)], half_in[0].at[rows_of(q)], half_recv[0].at[q], me + 3)

    def zero_relay(q):
        return side(1, q, main_in[2].at[rows_of(q)], wide_in.at[rows_of(q)], wide_recv.at[q], me + 5)

    def zero_down(q):
        return side(2, q, other.at[rows_of(q + HALF)], half_in[1].at[rows_of(q)], half_recv[1].at[q], me - 8)

    @pl.when(role == 0)
    def _():
        wait_pair()

        @pl.when(has_down)
        def _():
            @pl.loop(0, HALF)
            def _(q):
                zero_down(q).start()

        diagonal()

        def pass_on(q):
            @pl.when(has_up)
            def _():
                wait_main(2, q)
                zero_relay(q).start()

        @pl.loop(0, HALF)
        def _(q):
            rows = rows_of(q)
            wait_main(1, q)
            stage[rows, :] = jnp.where(whole, own[rows_of(q + HALF), :], main_in[1][rows, :])
            zero_side(q).start()
            pass_on(q)

        @pl.loop(HALF, PIECES)
        def _(q):
            wait_main(1, q)
            pass_on(q)

        @pl.loop(0, half_tiles)
        def _(p):
            both(lambda q: wait_half(0, q), p)
            left = half_in[0][rows_of(p, tile), :]
            meet(left, [(main_in[1][...], same(5, 7), 2, everywhere)], 3, p, half)

            @pl.when(has_up)
            def _():
                meet(left, [(main_in[2][...], same(7, 8), 4, everywhere)], 3, p, half)

        @pl.loop(0, half_tiles)
        def _(j):
            @pl.loop(3 * j, 3 + j)
            def _(p):
                both(lambda q: wait_main(0, q), p)
                meet(main_in[0][rows_of(p, tile), :],
                     [(own[...], same(0, 2), 0, everywhere), (main_in[1][...], same(2, 5), 2, everywhere)], 1, p)

            @pl.when(has_up)
            def _():
                both(lambda q: wait_half(1, q), j)
                meet(half_in[1][rows_of(j, tile), :], [(half_in[0][...], same(7, 9), 3, high_lanes)], 5, j, half)

        give(3, 7, 2)
        give(1, 2, 0)
        give(2, 5, 1)

        @pl.when(has_up)
        def _():
            give(4, 8, 4)
            give(5, 9, 2)

    def one_side(q):
        return side(0, q, stage.at[rows_of(q)], half_in[0].at[rows_of(q)], half_recv[0].at[q], me + 3)

    @pl.when(role == 1)
    def _():
        @pl.loop(0, HALF)
        def _(q):
            to_pair(q).wait_recv()
            rows = rows_of(q)
            stage[rows, :] = jnp.where(whole, other[rows, :], own[rows_of(q + HALF), :])
            one_side(q).start()

        diagonal()
        wait_pair(HALF, PIECES)
        pair_tile(same(0, 1))
        give(1, -1, 0)

    def two_down(q):
        return side(0, q, main_in[0].at[rows_of(q)], half_in[0].at[rows_of(q)], half_recv[0].at[q], me - 3)

    @pl.when(role == 2)
    def _():
        wait_pair()
        diagonal()
        from_four = same(1, 4) & jnp.logical_not(below)

        wait_wide(0)

        @pl.loop(0, HALF)
        def _(q):
            wait_main(0, q)

            @pl.when(has_down)
            def _():
                two_down(q).start()

        def first_block(p):
            meet(main_in[0][rows_of(p, tile), :],
                 [(own[...], same(1, 2), 0, everywhere), (other[...], same(1, 3), 2, everywhere)], 1, p)

        pl.loop(0, half_tiles)(first_block)
        pl.loop(1, HALF)(wait_wide)

        @pl.loop(0, half_tiles)
        def _(p):
            meet(wide_in[rows_of(p, tile), :],
                 [(own[...], below | same(2, 4), 0, everywhere),
                  (main_in[0][:half, :], from_four, 1, low_lanes)], 3, p)

        @pl.loop(half_tiles, tiles)
        def _(p):
            both(lambda q: wait_main(0, q), p)
            meet(main_in[0][rows_of(p, tile), :],
                 [(own[...], same(1, 2), 0, everywhere), (other[...], same(1, 3), 2, everywhere),
                  (wide_in[:half, :], from_four, 3, low_lanes)], 1, p)

        give(2, 1, 0)

        @pl.loop(half_tiles, tiles)
        def _(p):
            both(wait_wide, p)
            meet(wide_in[rows_of(p, tile), :],
                 [(own[...], below | same(2, 4), 0, everywhere),
                  (main_in[0][...], from_four, 1, everywhere)], 3, p)

        split(3, below, 5, everywhere, 4, everywhere, everywhere)
        give(1, -1, 0)
        give(4, 2, 1)

        @pl.when(has_down)
        def _():
            give(5, -3, 3)

    @pl.when(role == 3)
    def _():
        wait_pair()
        diagonal()
        pair_tile(same(2, 3))
        give(1, -1, 1)

        @pl.loop(0, half_tiles)
        def _(p):
            both(lambda q: wait_half(0, q), p)
            meet(half_in[0][rows_of(p, tile), :], [(own[...], whole | same(3, 5), 0, everywhere)], 2, p)

        split(2, whole, 3, high_lanes, 4, low_lanes, low_lanes)
        give(3, -3, 1)
        give(4, 2, 2)

    def four_side(q):
        return side(0, q, stage.at[rows_of(q)], half_in[0].at[rows_of(q)], half_recv[0].at[q], me + 2)

    def four_down(q):
        return side(1, q, half_in[0].at[rows_of(q)], half_in[1].at[rows_of(q)], half_recv[1].at[q], me - 7)

    @pl.when(role == 4)
    def _():
        wait_pair()
        diagonal()

        @pl.loop(0, HALF)
        def _(q):
            wait_half(0, q)

            @pl.when(has_down)
            def _():
                four_down(q).start()

            rows = rows_of(q)
            stage[rows, :] = jnp.where(whole, half_in[0][rows, :], other[rows_of(q + HALF), :])
            four_side(q).start()

        pair_tile(same(4, 5))
        give(1, 1, 0)

    @pl.when(role == 5)
    def _():
        wait_pair()
        diagonal()

        @pl.loop(0, tiles)
        def _(p):
            both(lambda q: wait_main(0, q), p)
            meet(main_in[0][rows_of(p, tile), :], [(own[...], same(5, 6), 0, everywhere)], 1, p)

        @pl.when(has_up)
        def _():
            @pl.loop(0, half_tiles)
            def _(p):
                both(lambda q: wait_half(1, q), p)
                meet(half_in[1][rows_of(p, tile), :], [(main_in[0][...], same(6, 9), 1, everywhere)], 4, p, half)

        @pl.loop(0, half_tiles)
        def _(p):
            @pl.when(has_up)
            def _():
                @pl.loop(2 * p, 2 + p)
                def _(i):
                    both(wait_wide, i)
                    meet(wide_in[rows_of(i, tile), :],
                         [(own[...], same(5, 8), 0, everywhere), (main_in[0][...], same(6, 8), 1, everywhere)], 3, i)

            both(lambda q: wait_half(0, q), p)
            left = half_in[0][rows_of(p, tile), :]
            meet(left, [(own[...], same(5, 7), 0, everywhere)], 2, p)

            @pl.when(has_up)
            def _():
                meet(left, [(half_in[1][...], same(7, 9), 4, high_lanes)], 2, p)

        @pl.when(has_up)
        def _():
            early = block - tile

            @pl.loop(0, half_tiles)
            def _(p):
                meet(half_in[0][rows_of(p, tile), :],
                     [(wide_in[:early, :], same(7, 8), 3, slice(0, early))], 2, p)

            both(wait_wide, tiles - 1)
            meet(wide_in[early:, :],
                 [(own[...], same(5, 8), 0, everywhere), (main_in[0][...], same(6, 8), 1, everywhere),
                  (half_in[0][...], same(7, 8), 2, low_lanes)], 3, tiles - 1)
            give(3, 3, 3)
            give(4, 4, 1)

        give(2, 2, 1)
        give(1, 1, 0)

    def six_side(q):
        return side(0, q, stage.at[rows_of(q)], wide_in.at[rows_of(q)], wide_recv.at[q], me - 4)

    def six_low(q):
        return side(1, q, other.at[rows_of(q)], half_in[0].at[rows_of(q)], half_recv[0].at[q], me - 1)

    @pl.when(role == 6)
    def _():
        wait_pair()

        @pl.loop(0, HALF)
        def _(q):
            six_low(q).start()

        diagonal()

        def choose(q):
            rows = rows_of(q)
            wait_main(0, q)

            @pl.when(has_down)
            def _():
                wait_main(2, q)
                stage[rows, :] = jnp.where(below, main_in[2][rows, :], main_in[0][rows, :])

            @pl.when(jnp.logical_not(has_down))
            def _():
                stage[rows, :] = main_in[0][rows, :]

            six_side(q).start()

        @pl.loop(0, tiles)
        def _(p):
            both(choose, p)
            meet(main_in[0][rows_of(p, tile), :],
                 [(own[...], same(4, 6), 0, everywhere), (other[...], same(4, 7), 2, everywhere)], 1, p)

        give(2, 1, 0)

        @pl.loop(0, tiles)
        def _(p):
            both(lambda q: wait_main(1, q), p)
            meet(main_in[1][rows_of(p, tile), :],
                 [(own[...], same(3, 6), 0, everywhere), (main_in[0][...], same(3, 4), 1, everywhere)], 3, p)

        give(1, -2, 0)

        @pl.loop(0, half_tiles)
        def _(p):
            both(lambda q: wait_half(0, q), p)
            meet(half_in[0][rows_of(p, tile), :], [(main_in[1][...], whole | same(3, 5), 3, everywhere)], 4, p)

        split(4, whole, 5, low_lanes, 6, high_lanes, low_lanes)
        give(3, -3, 1)
        give(5, -6, 2)
        give(6, -1, 3)

    @pl.when(role == 7)
    def _():
        wait_pair()
        diagonal()
        pair_tile(same(6, 7))

        @pl.when(has_up)
        def _():
            @pl.loop(0, half_tiles)
            def _(p):
                both(lambda q: wait_half(0, q), p)
                meet(half_in[0][rows_of(p, tile), :],
                     [(own[...], same(7, 9), 0, everywhere), (other[...], same(6, 9), 1, everywhere)], 2, p)

            give(2, 2, 3)

        give(1, -1, 1)

    def take(*places):
        for place in places:
            ret(0, 0, place).wait_recv()
            raise_to(0, everywhere, ret_in[place][...])

    expected = ((0, 1, 2), (0,), (0, 1), (0, 1), (0, 1), (0, 1, 2, 3), (0, 1), (0, 1, 2))
    for r in range(GROUP):
        @pl.when(role == r)
        def _():
            take(*expected[r])

    @pl.when(has_down & (role == 0))
    def _():
        take(3, 4)

    @pl.when(has_down & (role == 1))
    def _():
        take(1, 2, 3)

    @pl.when(has_up & (role == 7))
    def _():
        take(3)

    out_ref[...] = acc[0]

    @pl.loop(0, PIECES)
    def _(q):
        to_pair(q).wait_send()

        for_main(lambda r: to_main(r, q).wait_send())

        @pl.when((role == 0) & has_up)
        def _():
            zero_relay(q).wait_send()

        @pl.when(role == 6)
        def _():
            six_side(q).wait_send()

    @pl.loop(0, HALF)
    def _(q):
        @pl.when(role == 0)
        def _():
            zero_side(q).wait_send()

            @pl.when(has_down)
            def _():
                zero_down(q).wait_send()

        @pl.when(role == 1)
        def _():
            one_side(q).wait_send()

        @pl.when((role == 2) & has_down)
        def _():
            two_down(q).wait_send()

        @pl.when(role == 4)
        def _():
            four_side(q).wait_send()

            @pl.when(has_down)
            def _():
                four_down(q).wait_send()

        @pl.when(role == 6)
        def _():
            six_low(q).wait_send()

        @pl.when(role == 7)
        def _():
            high_half(q + HALF).wait_send()

    sent = ((1, 2, 3), (1,), (1, 2, 4), (1, 3, 4), (1,), (1, 2), (1, 2, 3, 5, 6), (1,))
    sent_up = ((4, 5), (), (), (), (), (3, 4), (), (2,))
    for r in range(GROUP):
        @pl.when(role == r)
        def _():
            for slot in sent[r]:
                ret(slot, 0, 0).wait_send()

            @pl.when(has_up)
            def _():
                for slot in sent_up[r]:
                    ret(slot, 0, 0).wait_send()

    @pl.when((role == 2) & has_down)
    def _():
        ret(5, 0, 0).wait_send()


def shards(sizes, embeddings, cluster_blocks):
    block, width = embeddings.shape
    wide = pltpu.VMEM((block, width), jnp.bfloat16)
    half = pltpu.VMEM((block // 2, width), jnp.bfloat16)
    line = pltpu.VMEM((1, block), jnp.float32)
    flags = pltpu.SemaphoreType.DMA((PIECES,))
    lone = pltpu.SemaphoreType.DMA
    out = pl.pallas_call(
        functools.partial(nearest_kernel, sizes),
        out_shape=pltpu.VMEM((1, block), jnp.float32),
        in_specs=[pl.BlockSpec(memory_space=pl.ANY)] * 2,
        out_specs=pl.BlockSpec(memory_space=pltpu.VMEM),
        scratch_shapes=[
            wide, wide, wide, wide, wide,
            pltpu.VMEM((8, 1, block), jnp.float32),
            wide, wide, wide, half, half, *[line] * 11, *[flags] * 8,
            flags, flags, flags, flags, flags,
            pltpu.SemaphoreType.DMA((7,)), pltpu.SemaphoreType.DMA((5,)),
            pltpu.SMEM(cluster_blocks.shape, jnp.int32), lone,
        ],
        compiler_params=pltpu.CompilerParams(collective_id=0, has_side_effects=True),
        name="nearest",
    )(cluster_blocks, embeddings)
    return out.reshape(-1)


def solution(mesh):
    sizes = (mesh.shape["rows"], mesh.shape["bal"])
    return jax.shard_map(
        functools.partial(shards, sizes), mesh=mesh,
        in_specs=(P(("rows", "bal"), None), P()), out_specs=P(("rows", "bal")), check_vma=False)
```

```python
import functools

import jax
import jax.numpy as jnp
from jax import lax
from jax.experimental import pallas as pl
from jax.experimental.pallas import tpu as pltpu
from jax.sharding import PartitionSpec as P

EPSILON = 1e-06
LOW = -2.0
MESH_ID = pl.DeviceIdType.MESH
PIECES = 4
HALF = PIECES // 2
GROUP = 8

NEAR = ((0, 1), (1, 0), (2, 3), (3, 2), (4, 5), (5, 4), (6, 7), (7, 6),
        (0, 2), (0, 5), (0, 7), (2, 1), (2, 6), (3, 0), (4, 1), (5, 6), (6, 3), (6, 4))
UPWARD = ((0, 0), (5, 4))
DOWNWARD = ((6, 7),)
MAIN_OFFSET = (-8, 1, -2, 3, 2, -5, -1, 7)
MAIN_SLOT = (2, 0, 0, 1, 0, 1, 0, 2)
FIRST_SEEN, LAST_SEEN = -1, 9


def nearest_kernel(sizes, counts_hbm, x_ref, out_ref, raw, own, other, wide_in, stage, acc, *rest):
    rest = list(rest)

    def several(many):
        return [rest.pop(0) for _ in range(many)]

    main_in, half_in, ret_in, lines = several(3), several(2), several(5), [None] + several(6)
    main_recv, half_recv, side_send = several(3), several(2), several(3)
    (load_sem, pair_send, pair_recv, main_send, wide_recv, ret_send, ret_recv,
     counts_ref, counts_sem) = rest
    n_rows, n_bal = sizes
    total = n_rows * n_bal
    block, width = x_ref.shape
    piece = block // PIECES
    tile = block // 4
    half = block // 2
    me = lax.axis_index("rows") * n_bal + lax.axis_index("bal")
    role = lax.rem(me, GROUP)
    base = me - role
    has_up = base + GROUP < total
    has_down = base > 0
    partner = me + 1 - 2 * lax.rem(me, 2)

    def coords(index):
        return (index // n_bal, lax.rem(index, n_bal))

    def by_role(values):
        return sum((role == place).astype(jnp.int32) * value for place, value in enumerate(values))

    barrier = pltpu.get_barrier_semaphore()
    def told_by(edges, r):
        return [there for here, there in edges if here == r]

    def heard_by(edges):
        return by_role([sum(there == r for _, there in edges) for r in range(GROUP)])

    def greet(index):
        pl.semaphore_signal(barrier, inc=1, device_id=coords(index), device_id_type=MESH_ID)

    for r in range(GROUP):
        @pl.when(role == r)
        def _():
            for there in told_by(NEAR, r):
                greet(me + there - r)

            for edges, exists, step in ((UPWARD, has_up, GROUP), (DOWNWARD, has_down, -GROUP)):
                if told_by(edges, r):
                    @pl.when(exists)
                    def _():
                        for there in told_by(edges, r):
                            greet(me + step + there - r)

    greeted = (heard_by(NEAR) + has_down.astype(jnp.int32) * heard_by(UPWARD)
               + has_up.astype(jnp.int32) * heard_by(DOWNWARD))

    def rows_of(q, size=piece):
        return pl.ds(pl.multiple_of(q * size, size), size)

    def load(q):
        return pltpu.make_async_copy(x_ref.at[rows_of(q)], raw.at[rows_of(q)], load_sem.at[q])

    counts_load = pltpu.make_async_copy(counts_hbm, counts_ref, counts_sem)
    counts_load.start()

    @pl.loop(0, PIECES)
    def _(q):
        load(q).start()

    def copy_to(src, dst, send, recv, index):
        return pltpu.make_async_remote_copy(
            src_ref=src, dst_ref=dst, send_sem=send, recv_sem=recv,
            device_id=coords(index), device_id_type=MESH_ID)

    def to_main(r, q):
        slot = MAIN_SLOT[r]
        return copy_to(own.at[rows_of(q)], main_in[slot].at[rows_of(q)],
                       main_send.at[q], main_recv[slot].at[q], me + MAIN_OFFSET[r])

    def for_main(act):
        for r in range(GROUP):
            here = role == r
            if r == 0:
                here = here & has_down
            if r == 7:
                here = here & has_up
            pl.when(here)(functools.partial(act, r))

    def to_pair(q):
        return copy_to(own.at[rows_of(q)], other.at[rows_of(q)], pair_send.at[q], pair_recv.at[q], partner)

    def side(slot, q, src, dst, recv, index):
        return copy_to(src, dst, side_send[slot].at[q], recv, index)

    def high_half(q):
        low = q - HALF
        return side(0, low, own.at[rows_of(q)], half_in[0].at[rows_of(low)], half_recv[0].at[low], me - 7)

    def normalise(q):
        rows = rows_of(q)
        load(q).wait()
        values = raw[rows, :].astype(jnp.float32)
        scale = lax.rsqrt(jnp.sum(values * values, axis=1, keepdims=True) + EPSILON)
        own[rows, :] = (values * scale).astype(jnp.bfloat16)

    def send(q):
        to_pair(q).start()

        for_main(lambda r: to_main(r, q).start())

        @pl.when((role == 7) & (q >= HALF))
        def _():
            high_half(q).start()


    pl.loop(0, HALF)(normalise)
    pl.semaphore_wait(barrier, greeted)
    pl.loop(0, HALF)(send)

    @pl.loop(HALF, PIECES)
    def _(q):
        normalise(q)
        send(q)

    counts_load.wait()

    def count(i, carry):
        end, owners = carry
        end = end + counts_ref[i]
        return end, tuple(
            owner + (end <= base + place).astype(jnp.int32)
            for place, owner in zip(range(FIRST_SEEN, LAST_SEEN + 1), owners))

    zero = jnp.int32(0)
    _, owners = lax.fori_loop(0, counts_ref.shape[0], count,
                              (zero, (zero,) * (LAST_SEEN + 1 - FIRST_SEEN)))

    def same(i, j):
        return owners[i - FIRST_SEEN] == owners[j - FIRST_SEEN]

    whole = same(0, 3)
    below = same(-1, 2) & has_down
    acc[...] = jnp.full(acc.shape, LOW, jnp.float32)

    def products(left, right):
        return lax.dot_general(left, right, (((1,), (1,)), ((), ())),
                               preferred_element_type=jnp.float32)

    def lanes_max(values):
        highest = values[:, :128]
        for start in range(128, values.shape[1], 128):
            highest = jnp.maximum(highest, values[:, start:start + 128])
        return highest

    def raise_to(slot, lanes, top):
        acc[slot, :, lanes] = jnp.maximum(acc[slot, :, lanes], top)

    everywhere = slice(None)
    low_lanes = slice(0, half)
    high_lanes = slice(half, block)

    def meet(left, partners, row_slot, p, shift=0):
        part = None
        for right, permitted, column_slot, lanes in partners:
            values = products(left, right)
            top = jnp.max(values, axis=0, keepdims=True)
            raise_to(column_slot, lanes, jnp.where(permitted, top, LOW))
            across = jnp.where(permitted, lanes_max(values), LOW)
            part = across if part is None else jnp.maximum(part, across)
        lanes = pl.ds(pl.multiple_of(p * tile + shift, tile), tile)
        raise_to(row_slot, lanes, jnp.max(part.T, axis=0, keepdims=True))

    def diagonal():
        @pl.loop(0, block // tile)
        def _(p):
            values = products(own[rows_of(p, tile), :], own[...])
            across = lax.broadcasted_iota(jnp.int32, values.shape, 1)
            down = lax.broadcasted_iota(jnp.int32, values.shape, 0) + p * tile
            values = jnp.where(across == down, LOW, values)
            raise_to(0, everywhere, jnp.max(values, axis=0, keepdims=True))

    def pair_tile(permitted):
        @pl.loop(0, block // tile)
        def _(p):
            meet(other[rows_of(p, tile), :], [(own[...], permitted, 0, everywhere)], 1, p)

    def wait_pair(begin=0, end=PIECES):
        @pl.loop(begin, end)
        def _(q):
            to_pair(q).wait_recv()

    def wait_main(slot, q):
        copy_to(own.at[rows_of(q)], main_in[slot].at[rows_of(q)],
                main_send.at[q], main_recv[slot].at[q], me).wait_recv()

    def wait_wide(q):
        side(0, q, stage.at[rows_of(q)], wide_in.at[rows_of(q)], wide_recv.at[q], me).wait_recv()

    def wait_half(slot, q):
        side(0, q, stage.at[rows_of(q)], half_in[slot].at[rows_of(q)], half_recv[slot].at[q], me).wait_recv()

    def both(wait, p):
        many = tile // piece
        for k in range(many):
            wait(many * p + k)

    def ret(slot, offset, place):
        return copy_to(lines[max(slot, 1)], ret_in[place], ret_send.at[slot], ret_recv.at[place], me + offset)

    def give(slot, offset, place):
        lines[slot][...] = acc[slot]
        ret(slot, offset, place).start()

    tiles = block // tile
    half_tiles = half // tile

    def split(slot, chosen, first_slot, first_lanes, second_slot, second_lanes, lanes):
        acc[first_slot, :, first_lanes] = jnp.where(chosen, acc[slot, :, lanes], LOW)
        acc[second_slot, :, second_lanes] = jnp.where(chosen, LOW, acc[slot, :, lanes])

    def zero_side(q):
        return side(0, q, stage.at[rows_of(q)], half_in[0].at[rows_of(q)], half_recv[0].at[q], me + 3)

    def zero_relay(q):
        return side(1, q, main_in[2].at[rows_of(q)], wide_in.at[rows_of(q)], wide_recv.at[q], me + 5)

    def zero_down(q):
        return side(2, q, other.at[rows_of(q + HALF)], half_in[1].at[rows_of(q)], half_recv[1].at[q], me - 8)

    @pl.when(role == 0)
    def _():
        wait_pair()

        @pl.when(has_down)
        def _():
            @pl.loop(0, HALF)
            def _(q):
                zero_down(q).start()

        diagonal()

        def pass_on(q):
            @pl.when(has_up)
            def _():
                wait_main(2, q)
                zero_relay(q).start()

        @pl.loop(0, HALF)
        def _(q):
            rows = rows_of(q)
            wait_main(1, q)
            stage[rows, :] = jnp.where(whole, own[rows_of(q + HALF), :], main_in[1][rows, :])
            zero_side(q).start()
            pass_on(q)

        @pl.loop(HALF, PIECES)
        def _(q):
            wait_main(1, q)
            pass_on(q)

        @pl.loop(0, half_tiles)
        def _(p):
            both(lambda q: wait_half(0, q), p)
            left = half_in[0][rows_of(p, tile), :]
            meet(left, [(main_in[1][...], same(5, 7), 2, everywhere)], 3, p, half)

            @pl.when(has_up)
            def _():
                meet(left, [(main_in[2][...], same(7, 8), 4, everywhere)], 3, p, half)

        @pl.loop(0, half_tiles)
        def _(j):
            @pl.loop(3 * j, 3 + j)
            def _(p):
                both(lambda q: wait_main(0, q), p)
                meet(main_in[0][rows_of(p, tile), :],
                     [(own[...], same(0, 2), 0, everywhere), (main_in[1][...], same(2, 5), 2, everywhere)], 1, p)

            @pl.when(has_up)
            def _():
                both(lambda q: wait_half(1, q), j)
                meet(half_in[1][rows_of(j, tile), :], [(half_in[0][...], same(7, 9), 3, high_lanes)], 5, j, half)

        give(3, 7, 2)
        give(1, 2, 0)
        give(2, 5, 1)

        @pl.when(has_up)
        def _():
            give(4, 8, 4)
            give(5, 9, 2)

    def one_side(q):
        return side(0, q, stage.at[rows_of(q)], half_in[0].at[rows_of(q)], half_recv[0].at[q], me + 3)

    @pl.when(role == 1)
    def _():
        @pl.loop(0, HALF)
        def _(q):
            to_pair(q).wait_recv()
            rows = rows_of(q)
            stage[rows, :] = jnp.where(whole, other[rows, :], own[rows_of(q + HALF), :])
            one_side(q).start()

        diagonal()
        wait_pair(HALF, PIECES)
        pair_tile(same(0, 1))
        give(1, -1, 0)

    def two_down(q):
        return side(0, q, main_in[0].at[rows_of(q)], half_in[0].at[rows_of(q)], half_recv[0].at[q], me - 3)

    @pl.when(role == 2)
    def _():
        wait_pair()
        diagonal()
        from_four = same(1, 4) & jnp.logical_not(below)

        wait_wide(0)

        @pl.loop(0, HALF)
        def _(q):
            wait_main(0, q)

            @pl.when(has_down)
            def _():
                two_down(q).start()

        def first_block(p):
            meet(main_in[0][rows_of(p, tile), :],
                 [(own[...], same(1, 2), 0, everywhere), (other[...], same(1, 3), 2, everywhere)], 1, p)

        pl.loop(0, half_tiles)(first_block)
        pl.loop(1, HALF)(wait_wide)

        @pl.loop(0, half_tiles)
        def _(p):
            meet(wide_in[rows_of(p, tile), :],
                 [(own[...], below | same(2, 4), 0, everywhere),
                  (main_in[0][:half, :], from_four, 1, low_lanes)], 3, p)

        @pl.loop(half_tiles, tiles)
        def _(p):
            both(lambda q: wait_main(0, q), p)
            meet(main_in[0][rows_of(p, tile), :],
                 [(own[...], same(1, 2), 0, everywhere), (other[...], same(1, 3), 2, everywhere),
                  (wide_in[:half, :], from_four, 3, low_lanes)], 1, p)

        give(2, 1, 0)

        @pl.loop(half_tiles, tiles)
        def _(p):
            both(wait_wide, p)
            meet(wide_in[rows_of(p, tile), :],
                 [(own[...], below | same(2, 4), 0, everywhere),
                  (main_in[0][...], from_four, 1, everywhere)], 3, p)

        split(3, below, 5, everywhere, 4, everywhere, everywhere)
        give(1, -1, 0)
        give(4, 2, 1)

        @pl.when(has_down)
        def _():
            give(5, -3, 3)

    @pl.when(role == 3)
    def _():
        wait_pair()
        diagonal()
        pair_tile(same(2, 3))
        give(1, -1, 1)

        @pl.loop(0, half_tiles)
        def _(p):
            both(lambda q: wait_half(0, q), p)
            meet(half_in[0][rows_of(p, tile), :], [(own[...], whole | same(3, 5), 0, everywhere)], 2, p)

        split(2, whole, 3, high_lanes, 4, low_lanes, low_lanes)
        give(3, -3, 1)
        give(4, 2, 2)

    def four_side(q):
        return side(0, q, stage.at[rows_of(q)], half_in[0].at[rows_of(q)], half_recv[0].at[q], me + 2)

    def four_down(q):
        return side(1, q, half_in[0].at[rows_of(q)], half_in[1].at[rows_of(q)], half_recv[1].at[q], me - 7)

    @pl.when(role == 4)
    def _():
        wait_pair()
        diagonal()

        @pl.loop(0, HALF)
        def _(q):
            wait_half(0, q)

            @pl.when(has_down)
            def _():
                four_down(q).start()

            rows = rows_of(q)
            stage[rows, :] = jnp.where(whole, half_in[0][rows, :], other[rows_of(q + HALF), :])
            four_side(q).start()

        pair_tile(same(4, 5))
        give(1, 1, 0)

    @pl.when(role == 5)
    def _():
        wait_pair()
        diagonal()

        @pl.loop(0, tiles)
        def _(p):
            both(lambda q: wait_main(0, q), p)
            meet(main_in[0][rows_of(p, tile), :], [(own[...], same(5, 6), 0, everywhere)], 1, p)

        @pl.when(has_up)
        def _():
            @pl.loop(0, half_tiles)
            def _(p):
                both(lambda q: wait_half(1, q), p)
                meet(half_in[1][rows_of(p, tile), :], [(main_in[0][...], same(6, 9), 1, everywhere)], 4, p, half)

        @pl.loop(0, half_tiles)
        def _(p):
            @pl.when(has_up)
            def _():
                @pl.loop(2 * p, 2 + p)
                def _(i):
                    both(wait_wide, i)
                    meet(wide_in[rows_of(i, tile), :],
                         [(own[...], same(5, 8), 0, everywhere), (main_in[0][...], same(6, 8), 1, everywhere)], 3, i)

            both(lambda q: wait_half(0, q), p)
            left = half_in[0][rows_of(p, tile), :]
            meet(left, [(own[...], same(5, 7), 0, everywhere)], 2, p)

            @pl.when(has_up)
            def _():
                meet(left, [(half_in[1][...], same(7, 9), 4, high_lanes)], 2, p)

        @pl.when(has_up)
        def _():
            early = block - tile

            @pl.loop(0, half_tiles)
            def _(p):
                meet(half_in[0][rows_of(p, tile), :],
                     [(wide_in[:early, :], same(7, 8), 3, slice(0, early))], 2, p)

            both(wait_wide, tiles - 1)
            meet(wide_in[early:, :],
                 [(own[...], same(5, 8), 0, everywhere), (main_in[0][...], same(6, 8), 1, everywhere),
                  (half_in[0][...], same(7, 8), 2, low_lanes)], 3, tiles - 1)
            give(3, 3, 3)
            give(4, 4, 1)

        give(2, 2, 1)
        give(1, 1, 0)

    def six_side(q):
        return side(0, q, stage.at[rows_of(q)], wide_in.at[rows_of(q)], wide_recv.at[q], me - 4)

    def six_low(q):
        return side(1, q, other.at[rows_of(q)], half_in[0].at[rows_of(q)], half_recv[0].at[q], me - 1)

    @pl.when(role == 6)
    def _():
        wait_pair()

        @pl.loop(0, HALF)
        def _(q):
            six_low(q).start()

        diagonal()

        def choose(q):
            rows = rows_of(q)
            wait_main(0, q)

            @pl.when(has_down)
            def _():
                wait_main(2, q)
                stage[rows, :] = jnp.where(below, main_in[2][rows, :], main_in[0][rows, :])

            @pl.when(jnp.logical_not(has_down))
            def _():
                stage[rows, :] = main_in[0][rows, :]

            six_side(q).start()

        @pl.loop(0, tiles)
        def _(p):
            both(choose, p)
            meet(main_in[0][rows_of(p, tile), :],
                 [(own[...], same(4, 6), 0, everywhere), (other[...], same(4, 7), 2, everywhere)], 1, p)

        give(2, 1, 0)

        @pl.loop(0, tiles)
        def _(p):
            both(lambda q: wait_main(1, q), p)
            meet(main_in[1][rows_of(p, tile), :],
                 [(own[...], same(3, 6), 0, everywhere), (main_in[0][...], same(3, 4), 1, everywhere)], 3, p)

        give(1, -2, 0)

        @pl.loop(0, half_tiles)
        def _(p):
            both(lambda q: wait_half(0, q), p)
            meet(half_in[0][rows_of(p, tile), :], [(main_in[1][...], whole | same(3, 5), 3, everywhere)], 4, p)

        split(4, whole, 5, low_lanes, 6, high_lanes, low_lanes)
        give(3, -3, 1)
        give(5, -6, 2)
        give(6, -1, 3)

    @pl.when(role == 7)
    def _():
        wait_pair()
        diagonal()
        pair_tile(same(6, 7))

        @pl.when(has_up)
        def _():
            @pl.loop(0, half_tiles)
            def _(p):
                both(lambda q: wait_half(0, q), p)
                meet(half_in[0][rows_of(p, tile), :],
                     [(own[...], same(7, 9), 0, everywhere), (other[...], same(6, 9), 1, everywhere)], 2, p)

            give(2, 2, 3)

        give(1, -1, 1)

    def take(*places):
        for place in places:
            ret(0, 0, place).wait_recv()
            raise_to(0, everywhere, ret_in[place][...])

    expected = ((0, 1, 2), (0,), (0, 1), (0, 1), (0, 1), (0, 1, 2, 3), (0, 1), (0, 1, 2))
    for r in range(GROUP):
        @pl.when(role == r)
        def _():
            take(*expected[r])

    @pl.when(has_down & (role == 0))
    def _():
        take(3, 4)

    @pl.when(has_down & (role == 1))
    def _():
        take(1, 2, 3)

    @pl.when(has_up & (role == 7))
    def _():
        take(3)

    out_ref[...] = acc[0]

    @pl.loop(0, PIECES)
    def _(q):
        to_pair(q).wait_send()

        for_main(lambda r: to_main(r, q).wait_send())

        @pl.when((role == 0) & has_up)
        def _():
            zero_relay(q).wait_send()

        @pl.when(role == 6)
        def _():
            six_side(q).wait_send()

    @pl.loop(0, HALF)
    def _(q):
        @pl.when(role == 0)
        def _():
            zero_side(q).wait_send()

            @pl.when(has_down)
            def _():
                zero_down(q).wait_send()

        @pl.when(role == 1)
        def _():
            one_side(q).wait_send()

        @pl.when((role == 2) & has_down)
        def _():
            two_down(q).wait_send()

        @pl.when(role == 4)
        def _():
            four_side(q).wait_send()

            @pl.when(has_down)
            def _():
                four_down(q).wait_send()

        @pl.when(role == 6)
        def _():
            six_low(q).wait_send()

        @pl.when(role == 7)
        def _():
            high_half(q + HALF).wait_send()

    sent = ((1, 2, 3), (1,), (1, 2, 4), (1, 3, 4), (1,), (1, 2), (1, 2, 3, 5, 6), (1,))
    sent_up = ((4, 5), (), (), (), (), (3, 4), (), (2,))
    for r in range(GROUP):
        @pl.when(role == r)
        def _():
            for slot in sent[r]:
                ret(slot, 0, 0).wait_send()

            @pl.when(has_up)
            def _():
                for slot in sent_up[r]:
                    ret(slot, 0, 0).wait_send()

    @pl.when((role == 2) & has_down)
    def _():
        ret(5, 0, 0).wait_send()


def shards(sizes, embeddings, cluster_blocks):
    block, width = embeddings.shape
    wide = pltpu.VMEM((block, width), jnp.bfloat16)
    half = pltpu.VMEM((block // 2, width), jnp.bfloat16)
    line = pltpu.VMEM((1, block), jnp.float32)
    flags = pltpu.SemaphoreType.DMA((PIECES,))
    lone = pltpu.SemaphoreType.DMA
    out = pl.pallas_call(
        functools.partial(nearest_kernel, sizes),
        out_shape=pltpu.VMEM((1, block), jnp.float32),
        in_specs=[pl.BlockSpec(memory_space=pl.ANY)] * 2,
        out_specs=pl.BlockSpec(memory_space=pltpu.VMEM),
        scratch_shapes=[
            wide, wide, wide, wide, wide,
            pltpu.VMEM((8, 1, block), jnp.float32),
            wide, wide, wide, half, half, *[line] * 11, *[flags] * 8,
            flags, flags, flags, flags, flags,
            pltpu.SemaphoreType.DMA((7,)), pltpu.SemaphoreType.DMA((5,)),
            pltpu.SMEM(cluster_blocks.shape, jnp.int32), lone,
        ],
        compiler_params=pltpu.CompilerParams(collective_id=0, has_side_effects=True),
        name="nearest",
    )(cluster_blocks, embeddings)
    return out.reshape(-1)


def solution(mesh):
    sizes = (mesh.shape["rows"], mesh.shape["bal"])
    return jax.shard_map(
        functools.partial(shards, sizes), mesh=mesh,
        in_specs=(P(("rows", "bal"), None), P()), out_specs=P(("rows", "bal")), check_vma=False)
```
